8 devices in a mesh: tp: 2 (over z, y), cp: 4 (over x, core).
Axes of the slice: x: 2, y: 2, z: 1, core: 2. Of those that a mesh axis runs over, the one named last changes fastest.
Arguments:
- hidden: bfloat16 [16, 2048, 2048], P(None, 'cp')
- grad_out: bfloat16 [16, 2048, 2048], P(None, 'cp')
- w_query: bfloat16 [2048, 8, 256], P(None, 'tp')
- w_key: bfloat16 [2048, 256], replicated
- w_value: bfloat16 [2048, 256], replicated
- w_out: bfloat16 [8, 256, 2048], P('tp')
Outputs:
- output 1: bfloat16 [16, 2048, 2048], P(None, 'cp')
- output 2: bfloat16 [16, 2048, 2048], P(None, 'cp')
- output 3: float32 [2048, 8, 256], P(None, 'tp')
- output 4: float32 [2048, 256], replicated
- output 5: float32 [2048, 256], replicated
- output 6: float32 [8, 256, 2048], P('tp')
All inputs are finite; a program needn't handle non-finite values.
Results may differ from the reference program's by a relative error of at most 0.0110002.
Values are sent between devices in bfloat16 or wider.
A program may use at most 1 GiB of HBM per device.

```python
import jax
import jax.numpy as jnp
from jax import lax

BATCH = 16
SEQ = 2048
D_MODEL = 2048
HEADS = 8
HEAD_DIM = 256
Q_ROWS = 128


def rope_tables(positions):
    half_dim = HEAD_DIM // 2
    inv_freq = 1.0 / jnp.power(10000.0, jnp.arange(half_dim, dtype=jnp.float32) * (2.0 / HEAD_DIM))
    angles = positions.astype(jnp.float32)[:, None] * inv_freq[None, :]
    return jnp.cos(angles), jnp.sin(angles)


def rotate(rot_in, cos_tab, sin_tab):
    half_dim = rot_in.shape[-1] // 2
    low_half = rot_in[..., :half_dim]
    high_half = rot_in[..., half_dim:]
    return jnp.concatenate([low_half * cos_tab - high_half * sin_tab, high_half * cos_tab + low_half * sin_tab], axis=-1)


def unrotate(rot_in, cos_tab, sin_tab):
    half_dim = rot_in.shape[-1] // 2
    low_half = rot_in[..., :half_dim]
    high_half = rot_in[..., half_dim:]
    return jnp.concatenate([low_half * cos_tab + high_half * sin_tab, high_half * cos_tab - low_half * sin_tab], axis=-1)


def setup_inputs(seed: int = 0) -> dict:
    sub_keys = jax.random.split(jax.random.key(seed), 6)
    hidden = jax.random.normal(sub_keys[0], (BATCH, SEQ, D_MODEL), jnp.float32)
    grad_out = jax.random.normal(sub_keys[1], (BATCH, SEQ, D_MODEL), jnp.float32)
    in_scale = D_MODEL ** -0.5
    w_query = jax.random.normal(sub_keys[2], (D_MODEL, HEADS, HEAD_DIM), jnp.float32) * in_scale
    w_key = jax.random.normal(sub_keys[3], (D_MODEL, HEAD_DIM), jnp.float32) * in_scale
    w_value = jax.random.normal(sub_keys[4], (D_MODEL, HEAD_DIM), jnp.float32) * in_scale
    w_out = jax.random.normal(sub_keys[5], (HEADS, HEAD_DIM, D_MODEL), jnp.float32) * (HEADS * HEAD_DIM) ** -0.5
    return {"hidden": hidden.astype(jnp.bfloat16), "grad_out": grad_out.astype(jnp.bfloat16), "w_query": w_query.astype(jnp.bfloat16), "w_key": w_key.astype(jnp.bfloat16), "w_value": w_value.astype(jnp.bfloat16), "w_out": w_out.astype(jnp.bfloat16)}


def reference(hidden, grad_out, w_query, w_key, w_value, w_out):
    q_scale = HEAD_DIM ** -0.5
    n_blocks = SEQ // Q_ROWS
    cos_tab, sin_tab = rope_tables(jnp.arange(SEQ))
    flat_hidden = hidden.reshape(BATCH * SEQ, D_MODEL)
    key_pre = jnp.dot(flat_hidden, w_key, preferred_element_type=jnp.float32).reshape(BATCH, SEQ, HEAD_DIM)
    key_rot = rotate(key_pre, cos_tab, sin_tab).astype(jnp.bfloat16).astype(jnp.float32)
    val_all = jnp.dot(flat_hidden, w_value, preferred_element_type=jnp.float32).reshape(BATCH, SEQ, HEAD_DIM).astype(jnp.bfloat16).astype(jnp.float32)
    key_pos = jnp.arange(SEQ)
    hid_blocks = hidden.reshape(BATCH, n_blocks, Q_ROWS, D_MODEL).transpose(1, 0, 2, 3)
    grad_blocks = grad_out.reshape(BATCH, n_blocks, Q_ROWS, D_MODEL).transpose(1, 0, 2, 3)
    cos_blocks = cos_tab.reshape(n_blocks, Q_ROWS, HEAD_DIM // 2)
    sin_blocks = sin_tab.reshape(n_blocks, Q_ROWS, HEAD_DIM // 2)
    row_starts = jnp.arange(n_blocks) * Q_ROWS
    kv_zero = jnp.zeros((BATCH, SEQ, HEAD_DIM), jnp.float32)
    big_zero = jnp.zeros((BATCH, SEQ, D_MODEL), jnp.float32)

    def head_step(carry_in, head_weights):
        out_acc, dh_acc, dk_acc, dv_acc = carry_in
        wq_head, wo_head = head_weights

        def block_step(block_carry, block_in):
            dk_run, dv_run, dwq_run, dwo_run = block_carry
            hid_blk, grad_blk, cos_blk, sin_blk, row_start = block_in
            hid_flat = hid_blk.reshape(BATCH * Q_ROWS, D_MODEL)
            grad_flat = grad_blk.reshape(BATCH * Q_ROWS, D_MODEL)
            q_pre = jnp.dot(hid_flat, wq_head, preferred_element_type=jnp.float32).reshape(BATCH, Q_ROWS, HEAD_DIM)
            q_rot = (rotate(q_pre, cos_blk, sin_blk) * q_scale).astype(jnp.bfloat16).astype(jnp.float32)
            scores = jnp.einsum("bqe,bke->bqk", q_rot, key_rot)
            q_pos = row_start + jnp.arange(Q_ROWS)
            allowed = key_pos[None, :] <= q_pos[:, None]
            scores = jnp.where(allowed[None], scores, -jnp.inf)
            probs_blk = jax.nn.softmax(scores, axis=-1)
            attn_blk = jnp.einsum("bqk,bke->bqe", probs_blk, val_all).astype(jnp.bfloat16)
            d_attn = jnp.dot(grad_flat, wo_head.T, preferred_element_type=jnp.float32).astype(jnp.bfloat16)
            attn_f = attn_blk.astype(jnp.float32)
            d_attn_f = d_attn.astype(jnp.float32).reshape(BATCH, Q_ROWS, HEAD_DIM)
            d_prob = jnp.einsum("bqe,bke->bqk", d_attn_f, val_all)
            row_delta = jnp.sum(d_attn_f * attn_f, axis=-1, keepdims=True)
            d_score = probs_blk * (d_prob - row_delta)
            dq_blk = jnp.einsum("bqk,bke->bqe", d_score, key_rot)
            dk_run = dk_run + jnp.einsum("bqk,bqe->bke", d_score, q_rot)
            dv_run = dv_run + jnp.einsum("bqk,bqe->bke", probs_blk, d_attn_f)
            dq_pre = (unrotate(dq_blk, cos_blk, sin_blk) * q_scale).astype(jnp.bfloat16).reshape(BATCH * Q_ROWS, HEAD_DIM)
            attn_flat = attn_blk.reshape(BATCH * Q_ROWS, HEAD_DIM)
            dwq_run = dwq_run + jnp.dot(hid_flat.T, dq_pre, preferred_element_type=jnp.float32)
            dwo_run = dwo_run + jnp.dot(attn_flat.T, grad_flat, preferred_element_type=jnp.float32)
            out_part = jnp.dot(attn_flat, wo_head, preferred_element_type=jnp.float32)
            dh_part = jnp.dot(dq_pre, wq_head.T, preferred_element_type=jnp.float32)
            return (dk_run, dv_run, dwq_run, dwo_run), (out_part, dh_part)

        block_init = (kv_zero, kv_zero, jnp.zeros((D_MODEL, HEAD_DIM), jnp.float32), jnp.zeros((HEAD_DIM, D_MODEL), jnp.float32))
        block_out, block_ys = lax.scan(block_step, block_init, (hid_blocks, grad_blocks, cos_blocks, sin_blocks, row_starts))
        dk_run, dv_run, dwq_run, dwo_run = block_out
        out_parts, dh_parts = block_ys
        out_head = out_parts.reshape(n_blocks, BATCH, Q_ROWS, D_MODEL).transpose(1, 0, 2, 3).reshape(BATCH, SEQ, D_MODEL)
        dh_head = dh_parts.reshape(n_blocks, BATCH, Q_ROWS, D_MODEL).transpose(1, 0, 2, 3).reshape(BATCH, SEQ, D_MODEL)
        new_carry = (out_acc + out_head, dh_acc + dh_head, dk_acc + dk_run, dv_acc + dv_run)
        return new_carry, (dwq_run, dwo_run)

    head_init = (big_zero, big_zero, kv_zero, kv_zero)
    head_out, head_ys = lax.scan(head_step, head_init, (w_query.transpose(1, 0, 2), w_out))
    out_acc, dh_acc, dk_acc, dv_acc = head_out
    d_w_query = head_ys[0].transpose(1, 0, 2)
    d_w_out = head_ys[1]
    dk_pre = unrotate(dk_acc, cos_tab, sin_tab).astype(jnp.bfloat16).reshape(BATCH * SEQ, HEAD_DIM)
    dv_pre = dv_acc.astype(jnp.bfloat16).reshape(BATCH * SEQ, HEAD_DIM)
    d_w_key = jnp.dot(flat_hidden.T, dk_pre, preferred_element_type=jnp.float32)
    d_w_value = jnp.dot(flat_hidden.T, dv_pre, preferred_element_type=jnp.float32)
    dh_kv = jnp.dot(dk_pre, w_key.T, preferred_element_type=jnp.float32) + jnp.dot(dv_pre, w_value.T, preferred_element_type=jnp.float32)
    d_hidden = (dh_acc + dh_kv.reshape(BATCH, SEQ, D_MODEL)).astype(jnp.bfloat16)
    attn_out = out_acc.astype(jnp.bfloat16)
    return attn_out, d_hidden, d_w_query, d_w_key, d_w_value, d_w_out
```

```python
import functools

import jax
import jax.numpy as jnp
from jax import lax
from jax.experimental import pallas as pl
from jax.experimental.pallas import tpu as pltpu
from jax.sharding import PartitionSpec as P


ROPE_BASE = 10000.0
F32 = jnp.float32
BF16 = jnp.bfloat16
HPS = 2
HPF = 4
E = 256
S = 512
HALF = 256


def rope_tables(positions, head_dim):
    half_dim = head_dim // 2
    inv_freq = 1.0 / jnp.power(ROPE_BASE, jnp.arange(half_dim, dtype=F32) * (2.0 / head_dim))
    angles = positions.astype(F32)[:, None] * inv_freq[None, :]
    return jnp.cos(angles), jnp.sin(angles)


def rot(x, cos, sin):
    h = x.shape[-1] // 2
    a, b = x[..., :h], x[..., h:]
    return jnp.concatenate([a * cos - b * sin, b * cos + a * sin], axis=-1)


def unrot(x, cos, sin):
    h = x.shape[-1] // 2
    a, b = x[..., :h], x[..., h:]
    return jnp.concatenate([a * cos + b * sin, b * cos - a * sin], axis=-1)


def dot_nt(a, b):
    return lax.dot_general(a, b, (((1,), (1,)), ((), ())), preferred_element_type=F32)


def dot(a, b):
    return jnp.dot(a, b, preferred_element_type=F32)


def causal_keep(n):
    return lax.broadcasted_iota(jnp.int32, (n, n), 0) <= lax.broadcasted_iota(jnp.int32, (n, n), 1)


def piece_range(c):
    return jnp.where(c == 2, 1, 0), jnp.where(c < 2, c, 3)


def fwd_kernel(cp_ref, qpre_ref, cos_ref, sin_ref, core_ref, x_ref, xc_ref, own_ref, q_ref, o_ref, lse_ref, m_scr, l_scr, acc_scr, k_scr, vt_scr):
    c = cp_ref[0]
    lo, hi = piece_range(c)
    keep = causal_keep(HALF)
    cos, sin = cos_ref[...], sin_ref[...]

    @pl.when(pl.program_id(1) == 0)
    def _():
        for n, ref in enumerate((core_ref, x_ref, xc_ref, own_ref)):
            def load(n=n, ref=ref):
                k_scr[n] = ref[0, :, :E]
                vt_scr[n] = ref[0, :, E:].T

            if n == 3:
                load()
            else:
                pl.when((n >= lo) & (n < hi))(load)

    qs = []
    for hh in range(HPF):
        cols = slice(hh * E, (hh + 1) * E)
        q = (rot(qpre_ref[0, :, cols], cos, sin) * (E ** -0.5)).astype(BF16)
        q_ref[0, :, cols] = q
        qs.append(q)

    def diag_scores(hh):
        q, k_d = qs[hh], k_scr[3]
        s_a = jnp.where(keep, dot_nt(k_d[:HALF], q[:HALF]), -jnp.inf)
        s_b = dot_nt(k_d[:HALF], q[HALF:])
        s_c = jnp.where(keep, dot_nt(k_d[HALF:], q[HALF:]), -jnp.inf)
        return s_a, s_b, s_c

    def diag_rest(hh, scores):
        s_a, s_b, s_c = scores
        m_a = jnp.max(s_a, axis=0, keepdims=True)
        m_b = jnp.maximum(jnp.max(s_b, axis=0, keepdims=True), jnp.max(s_c, axis=0, keepdims=True))
        p_a = jnp.exp(s_a - m_a)
        p_b = jnp.exp(s_b - m_b)
        p_c = jnp.exp(s_c - m_b)
        m_scr[hh, :, :HALF] = m_a
        m_scr[hh, :, HALF:] = m_b
        l_scr[hh, :, :HALF] = jnp.sum(p_a, axis=0, keepdims=True)
        l_scr[hh, :, HALF:] = jnp.sum(p_b, axis=0, keepdims=True) + jnp.sum(p_c, axis=0, keepdims=True)
        vt_d = vt_scr[3]
        acc_scr[hh, :, :HALF] = dot(vt_d[:, :HALF], p_a.astype(BF16))
        acc_scr[hh, :, HALF:] = dot(vt_d[:, :HALF], p_b.astype(BF16)) + dot(vt_d[:, HALF:], p_c.astype(BF16))

    nxt = diag_scores(0)
    for hh in range(HPF):
        cur = nxt
        if hh + 1 < HPF:
            nxt = diag_scores(hh + 1)
        diag_rest(hh, cur)

    def step(j, carry):
        def scores(hh):
            return dot_nt(k_scr[j], q_ref[0, :, hh * E:(hh + 1) * E])

        nxt = scores(0)
        for hh in range(HPF):
            s = nxt
            if hh + 1 < HPF:
                nxt = scores(hh + 1)
            m_old = m_scr[hh]
            m_new = jnp.maximum(m_old, jnp.max(s, axis=0, keepdims=True))
            alpha = jnp.exp(m_old - m_new)
            p = jnp.exp(s - m_new)
            m_scr[hh] = m_new
            l_scr[hh] = l_scr[hh] * alpha + jnp.sum(p, axis=0, keepdims=True)
            acc_scr[hh] = acc_scr[hh] * alpha + dot(vt_scr[j], p.astype(BF16))
        return carry

    lax.fori_loop(lo, hi, step, 0)
    for hh in range(HPF):
        l = l_scr[hh]
        o_ref[0, :, hh * E:(hh + 1) * E] = (acc_scr[hh] * (1.0 / l)).astype(BF16).T
        lse_ref[0, hh] = m_scr[hh] + jnp.log(l)


def attn_fwd(cp_arr, q_pre, cos, sin, pieces, b0, nb):
    width = q_pre.shape[2]
    n_hp = width // (HPF * E)
    wide = pl.BlockSpec((1, S, HPF * E), lambda b, h, cp: (b, 0, h))
    wide_in = pl.BlockSpec((1, S, HPF * E), lambda b, h, cp: (b + b0, 0, h))
    tab = pl.BlockSpec((S, E // 2), lambda b, h, cp: (0, 0))
    kv_spec = pl.BlockSpec((1, S, 2 * E), lambda b, h, cp: (b + b0, 0, 0))
    return pl.pallas_call(
        fwd_kernel,
        grid_spec=pltpu.PrefetchScalarGridSpec(
            num_scalar_prefetch=1,
            grid=(nb, n_hp),
            in_specs=[wide_in, tab, tab] + [kv_spec] * 4,
            out_specs=[wide, wide, pl.BlockSpec((1, HPF, 1, S), lambda b, h, cp: (b, h, 0, 0))],
            scratch_shapes=[pltpu.VMEM((HPF, 1, S), F32), pltpu.VMEM((HPF, 1, S), F32), pltpu.VMEM((HPF, E, S), F32),
                            pltpu.VMEM((4, S, E), BF16), pltpu.VMEM((4, E, S), BF16)]),
        out_shape=[jax.ShapeDtypeStruct((nb, S, width), BF16), jax.ShapeDtypeStruct((nb, S, width), BF16),
                   jax.ShapeDtypeStruct((nb, n_hp * HPF, 1, S), F32)],
        compiler_params=pltpu.CompilerParams(dimension_semantics=("arbitrary", "arbitrary"), vmem_limit_bytes=56 * 1024 * 1024),
        cost_estimate=pl.CostEstimate(flops=nb * 8 * 4 * 4 * S * S * E, bytes_accessed=nb * S * width * 8, transcendentals=0),
        name="attn_fwd",
    )(cp_arr, q_pre, cos, sin, *pieces)


def bwd_kernel(with_dkv, cp_ref, q_ref, do_ref, o_ref, lse_ref, cos_ref, sin_ref, core_ref, x_ref, xc_ref, own_ref, *rest):
    if with_dkv:
        dq_ref, dcore_ref, dx_ref, dxc_ref, down_ref, dl_scr, dqt_scr, k_scr, v_scr, kt_scr, dkv_scr = rest
        outs = (dcore_ref, dx_ref, dxc_ref, down_ref)
    else:
        dq_ref, dl_scr, dqt_scr, k_scr, v_scr, kt_scr = rest
        outs = (None,) * 4
    c = cp_ref[0]
    lo, hi = piece_range(c)
    keep = causal_keep(HALF)

    def each_piece(fn):
        for n, pair in enumerate(zip((core_ref, x_ref, xc_ref, own_ref), outs)):
            if n == 3:
                fn(n, *pair)
            else:
                pl.when((n >= lo) & (n < hi))(functools.partial(fn, n, *pair))

    @pl.when(pl.program_id(1) == 0)
    def _():
        def load(n, ref, out):
            k_scr[n] = ref[0, :, :E]
            v_scr[n] = ref[0, :, E:]
            kt_scr[n] = ref[0, :, :E].T
            if with_dkv:
                dkv_scr[n] = jnp.zeros((2, S, E), F32)

        each_piece(load)

    def cols(hh):
        return slice(hh * E, (hh + 1) * E)

    def scores(hh, j, ks, qs):
        s = dot_nt(k_scr[j, ks], q_ref[0, qs, cols(hh)])
        dp = dot_nt(v_scr[j, ks], do_ref[0, qs, cols(hh)])
        return s, dp

    def work(hh, sc, qs, masked):
        s, dp = sc
        p = jnp.exp(s - lse_ref[0, hh, :, qs])
        if masked:
            p = jnp.where(keep, p, 0.0)
        ds = (p * (dp - dl_scr[hh, :, qs])).astype(BF16)
        return p.astype(BF16), ds

    def grads(hh, j, p, ds, ks, qs):
        dqt_scr[hh, :, qs] += dot(kt_scr[j, :, ks], ds)
        if with_dkv:
            return dot(ds, q_ref[0, qs, cols(hh)]), dot(p, do_ref[0, qs, cols(hh)])
        return None

    def block(j, ks, qs, masked):
        nxt = scores(0, j, ks, qs)
        tot = None
        for hh in range(HPS):
            cur = nxt
            if hh + 1 < HPS:
                nxt = scores(hh + 1, j, ks, qs)
            p, ds = work(hh, cur, qs, masked)
            got = grads(hh, j, p, ds, ks, qs)
            if with_dkv:
                tot = got if tot is None else (tot[0] + got[0], tot[1] + got[1])
        if with_dkv:
            dkv_scr[j, 0, ks] += tot[0]
            dkv_scr[j, 1, ks] += tot[1]

    for hh in range(HPS):
        prod = do_ref[0, :, cols(hh)].astype(F32) * o_ref[0, :, cols(hh)].astype(F32)
        prod = prod[:, :E // 2] + prod[:, E // 2:]
        dl_scr[hh] = jnp.sum(prod.T, axis=0, keepdims=True)
        dqt_scr[hh] = jnp.zeros((E, S), F32)

    first, second = slice(0, HALF), slice(HALF, S)
    block(3, first, first, True)
    block(3, first, second, False)
    block(3, second, second, True)

    def step(j, carry):
        block(j, slice(0, S), slice(0, S), False)
        return carry

    lax.fori_loop(lo, hi, step, 0)
    for hh in range(HPS):
        dq = dqt_scr[hh].T
        dq_ref[0, :, cols(hh)] = (unrot(dq, cos_ref[...], sin_ref[...]) * (E ** -0.5)).astype(BF16)

    if with_dkv:
        @pl.when(pl.program_id(1) == pl.num_programs(1) - 1)
        def _():
            def store(n, ref, out):
                out[0, :, :E] = dkv_scr[n, 0]
                out[0, :, E:] = dkv_scr[n, 1]

            each_piece(store)


def attn_bwd(cp_arr, q, do, o, lse, cos, sin, pieces, b0, with_dkv=True):
    nb, _, width = q.shape
    n_hp = width // (HPS * E)
    wide = pl.BlockSpec((1, S, HPS * E), lambda b, h, cp: (b, 0, h))
    wide_in = pl.BlockSpec((1, S, HPS * E), lambda b, h, cp: (b + b0, 0, h))
    tab = pl.BlockSpec((S, E // 2), lambda b, h, cp: (0, 0))
    kv_spec = pl.BlockSpec((1, S, 2 * E), lambda b, h, cp: (b + b0, 0, 0))
    out_specs = [wide] + [pl.BlockSpec((1, S, 2 * E), lambda b, h, cp: (b, 0, 0))] * 4
    out_shape = [jax.ShapeDtypeStruct((nb, S, width), BF16)] + [jax.ShapeDtypeStruct((nb, S, 2 * E), F32)] * 4
    scratch = [pltpu.VMEM((HPS, 1, S), F32), pltpu.VMEM((HPS, E, S), F32), pltpu.VMEM((4, S, E), BF16),
               pltpu.VMEM((4, S, E), BF16), pltpu.VMEM((4, E, S), BF16), pltpu.VMEM((4, 2, S, E), F32)]
    n_out = 5 if with_dkv else 1
    res = pl.pallas_call(
        functools.partial(bwd_kernel, with_dkv),
        grid_spec=pltpu.PrefetchScalarGridSpec(
            num_scalar_prefetch=1,
            grid=(nb, n_hp),
            in_specs=[wide, wide_in, wide, pl.BlockSpec((1, HPS, 1, S), lambda b, h, cp: (b, h, 0, 0)), tab, tab] + [kv_spec] * 4,
            out_specs=out_specs[:n_out],
            scratch_shapes=scratch if with_dkv else scratch[:5]),
        out_shape=out_shape[:n_out],
        compiler_params=pltpu.CompilerParams(dimension_semantics=("arbitrary", "arbitrary"), vmem_limit_bytes=60 * 1024 * 1024),
        cost_estimate=pl.CostEstimate(flops=nb * 8 * 10 * 4 * S * S * E, bytes_accessed=nb * S * width * 8, transcendentals=0),
        name="attn_bwd" if with_dkv else "attn_bwd_dq",
    )(cp_arr, q, do, o, lse, cos, sin, *pieces)
    return res if with_dkv else res[0]


N_CHUNK = 4
SEQUENCE = (("f", 0), ("f", 1), ("b", 0), ("f", 2), ("b", 1), ("f", 3), ("b", 2), ("b", 3))
FINISH_AFTER = {0: 3, 1: 5, 2: 7}


def blank_kernel(o_ref):
    del o_ref


def blank(shape, dtype):
    return pl.pallas_call(blank_kernel, out_shape=jax.ShapeDtypeStruct(shape, dtype), out_specs=pl.BlockSpec(memory_space=pl.ANY))()


def solution(mesh):
    axes = ("tp", "cp")
    dev = lambda t, c: t * 4 + c
    Y = [(dev(t, c), dev(1 - t, c)) for t in range(2) for c in range(4)]
    CORE = [(dev(t, c), dev(t, c ^ 1)) for t in range(2) for c in range(4)]
    X = [(dev(t, c), dev(t, c ^ 2)) for t in range(2) for c in range(4)]
    XUP = [(dev(t, c), dev(t, c + 2)) for t in range(2) for c in range(2)]
    XDN = [(dev(t, c + 2), dev(t, c)) for t in range(2) for c in range(2)]
    ODD_DN = [(dev(t, c + 1), dev(t, c)) for t in range(2) for c in (0, 2)]
    CORE_HI = [(dev(t, c), dev(t, c ^ 1)) for t in range(2) for c in (2, 3)]

    def perm(x, pairs):
        return lax.ppermute(x, axes, pairs)

    def ein(spec, a, b, dtype=F32):
        return jnp.einsum(spec, a, b, preferred_element_type=F32).astype(dtype)

    def body(hidden, grad_out, w_query, w_key, w_value, w_out):
        t = lax.axis_index("tp")
        c = lax.axis_index("cp")
        core = c % 2
        xc = c // 2
        even = core == 0
        n_batch, _, d = hidden.shape
        nb = n_batch // 2
        cb = nb // N_CHUNK
        cp_arr = c.astype(jnp.int32).reshape(1)
        cos, sin = rope_tables(c * S + jnp.arange(S), E)
        wq_own = w_query.reshape(d, -1)
        wo_own = w_out.reshape(-1, d)
        n_own = wq_own.shape[1]
        w_kv = jnp.concatenate([w_key, w_value], axis=1)

        def fetch(w):
            rows = w.shape[0] // 2
            got = perm(lax.dynamic_slice_in_dim(w, core * rows, rows, 0), Y)
            other = perm(got, CORE)
            return jnp.where(even, jnp.concatenate([got, other], 0), jnp.concatenate([other, got], 0))

        wq_oth = fetch(wq_own)
        wo_oth = fetch(wo_own)
        w_q = jnp.concatenate([wq_own, wq_oth], axis=1)
        w_o = jnp.concatenate([wo_own, wo_oth], axis=0)

        h_own = lax.dynamic_slice_in_dim(hidden, t * nb, nb, 0)
        g_own = lax.dynamic_slice_in_dim(grad_out, t * nb, nb, 0)
        kv_pre = ein("bsd,de->bse", h_own, w_kv)
        kv_own = jnp.concatenate([rot(kv_pre[..., :E], cos, sin), kv_pre[..., E:]], axis=-1).astype(BF16)
        kv_core = perm(kv_own, CORE)
        kv_x = perm(kv_own, XUP)
        kv_xc = perm(kv_x, CORE_HI)
        pieces = (kv_core, kv_x, kv_xc, kv_own)

        def place(buf, val, col):
            return lax.dynamic_update_slice_in_dim(buf, val, col, 2)

        q_pre = place(blank((nb, S, 2 * n_own), F32), ein("bsd,de->bse", h_own, wq_own), 0)
        d_o = place(blank((nb, S, 2 * n_own), BF16), ein("bsd,ed->bse", g_own, wo_own, BF16), 0)
        q_pre = place(q_pre, ein("bsd,de->bse", h_own, wq_oth), n_own)
        d_o = place(d_o, ein("bsd,ed->bse", g_own, wo_oth, BF16), n_own)

        attn_out = blank(hidden.shape, BF16)
        d_hidden = blank(hidden.shape, BF16)
        gots, goths, fwd, bwd, dkv_parts = {}, {}, {}, {}, {}

        def finish(i, after):
            nonlocal d_hidden, q_pre, d_o
            tot = bwd[i][1]
            if after is not None:
                tot, after = lax.optimization_barrier((tot, after))
            dkv_pre = jnp.concatenate([unrot(tot[..., :E], cos, sin), tot[..., E:]], axis=-1).astype(BF16)
            d_h = (ein("bse,de->bsd", bwd[i][0], w_q) + ein("bse,de->bsd", dkv_pre, w_kv)).astype(BF16)
            q_pre, d_o, d_h = lax.optimization_barrier((q_pre, d_o, d_h))
            goths[i] = perm(d_h, Y)
            d_hidden = lax.dynamic_update_slice_in_dim(d_hidden, d_h, t * nb + i * cb, 0)
            dkv_parts[i] = dkv_pre
            return after

        for pos, (kind, i) in enumerate(SEQUENCE):
            if kind == "f":
                fwd[i] = attn_fwd(cp_arr, q_pre, cos, sin, pieces, i * cb, cb)
                out = ein("bse,ed->bsd", fwd[i][1], w_o, BF16)
                gots[i] = perm(out, Y)
                attn_out = lax.dynamic_update_slice_in_dim(attn_out, out, t * nb + i * cb, 0)
            else:
                q, o, lse = fwd[i]
                dq, d_core, d_x, d_xc, d_mine = attn_bwd(cp_arr, q, d_o, o, lse, cos, sin, pieces, i * cb)
                down = perm(d_core, ODD_DN)
                swap = perm(d_xc, CORE_HI)
                from_x = perm(d_x + swap, XDN)
                bwd[i] = (dq, d_mine + down + from_x)
            for k, at in FINISH_AFTER.items():
                if at == pos:
                    if kind == "f":
                        fwd[i] = (fwd[i][0], finish(k, fwd[i][1]), fwd[i][2])
                    else:
                        bwd[i] = (finish(k, bwd[i][0]), bwd[i][1])

        def pick(x, i, n):
            rows = x.shape[0] // n
            return lax.dynamic_slice_in_dim(x, i * rows, rows, 0)

        def join(first, a, b):
            return jnp.where(first, jnp.concatenate([a, b], 0), jnp.concatenate([b, a], 0))

        def reduce_w(own, oth):
            own = pick(own, core, 2) + perm(pick(own, 1 - core, 2), CORE)
            oth = pick(oth, core, 2) + perm(pick(oth, 1 - core, 2), CORE)
            oth = pick(oth, xc, 2) + perm(pick(oth, 1 - xc, 2), X)
            own = pick(own, xc, 2) + perm(pick(own, 1 - xc, 2), X)
            part = own + perm(oth, Y)
            half = join(xc == 0, part, perm(part, X))
            return join(even, half, perm(half, CORE))

        o_all = jnp.concatenate([fwd[i][1] for i in range(N_CHUNK)], 0)
        dq_all = jnp.concatenate([bwd[i][0] for i in range(N_CHUNK)], 0)
        two = [ein("bse,bsd->ed", o_all[..., k * n_own:(k + 1) * n_own], g_own) for k in range(2)]
        d_w_out = reduce_w(*two).reshape(w_out.shape)
        h_own, dq_all, _ = lax.optimization_barrier((h_own, dq_all, d_o))
        two = [ein("bsd,bse->de", h_own, dq_all[..., k * n_own:(k + 1) * n_own]) for k in range(2)]
        finish(N_CHUNK - 1, None)
        for i in range(N_CHUNK):
            attn_out = lax.dynamic_update_slice_in_dim(attn_out, gots[i], (1 - t) * nb + i * cb, 0)
            d_hidden = lax.dynamic_update_slice_in_dim(d_hidden, goths[i], (1 - t) * nb + i * cb, 0)
        dkv_all = jnp.concatenate([dkv_parts[i] for i in range(N_CHUNK)], 0)
        d_w_query = reduce_w(*two).reshape(w_query.shape)
        d_w_kv = lax.psum(ein("bsd,bse->de", h_own, dkv_all), axes)
        return attn_out, d_hidden, d_w_query, d_w_kv[:, :E], d_w_kv[:, E:], d_w_out

    row = P(None, "cp", None)
    return jax.shard_map(body, mesh=mesh, in_specs=(row, row, P(None, "tp", None), P(), P(), P("tp", None, None)), out_specs=(row, row, P(None, "tp", None), P(), P(), P("tp", None, None)), check_vma=False)
```
